32 devices in a mesh: rows: 8 (over z, y), cols: 4 (over x, core).
Axes of the slice: x: 2, y: 2, z: 4, core: 2. Of those that a mesh axis runs over, the one named last changes fastest.
Arguments:
- grad_stack: float32 [256, 64, 2048], P(None, 'rows', 'cols'), may hold values from -6 to 6
- moment_stack: float32 [256, 64, 2048], P(None, 'rows', 'cols'), may hold values from -6 to 6
- weight_stack: float32 [256, 64, 2048], P(None, 'rows', 'cols'), may hold values from -0.1875 to 0.1875
Outputs:
- new_weights: float32 [256, 64, 2048], P(None, 'rows', 'cols')
- new_momentum: float32 [256, 64, 2048], P(None, 'rows', 'cols')
The draws below stay inside these ranges and needn't reach their ends.
All inputs are finite; a program needn't handle non-finite values.
Results may differ from the reference program's by a relative error of at most 0.0003.
Values sent between devices are 32-bit elements.
A program may use at most 128 MiB of HBM per device.

```python
import jax
import jax.numpy as jnp
from jax import lax

SIDE = 64
WIDE = 2048
MATS = 256
ITERS = 5


def block_levels(rng, extent, shards, least, high):
    loudness, own = 1.0, jax.random.fold_in(rng, 6)
    for axis_at, shards_of in shards:
        steps = jnp.exp(jax.random.uniform(jax.random.fold_in(own, axis_at), (shards_of,), jnp.float32, least / len(shards), high / len(shards)))
        loudness = loudness * jnp.repeat(steps, extent[axis_at] // shards_of).reshape([-1 if axis == axis_at else 1 for axis in range(len(extent))])
    return loudness


def centred(own_key, dims, spread, most, cuts=(), dtype=jnp.bfloat16):
    loudness = block_levels(own_key, dims, cuts, -0.22, 0.18) if cuts else 1.0
    array = jax.random.normal(own_key, dims, jnp.float32) * spread * loudness
    return jnp.minimum(jnp.maximum(array, -most), most).astype(dtype)


def setup_inputs(seed: int = 0) -> dict:
    key_list = jax.random.split(jax.random.key(seed), 4)
    return {
        "grad_stack": centred(key_list[0], (MATS, SIDE, WIDE), 1.0, 6.0, ((1, 8), (2, 4)), jnp.float32),
        "moment_stack": centred(key_list[1], (MATS, SIDE, WIDE), 1.0, 6.0, ((1, 8), (2, 4)), jnp.float32),
        "weight_stack": centred(key_list[2], (MATS, SIDE, WIDE), 0.03, 0.1875, ((1, 8), (2, 4)), jnp.float32),
    }


hold_rate = 0.95
learn_rate = 1.0

def reference(grad_stack, moment_stack, weight_stack):
    new_momentum = hold_rate * moment_stack + grad_stack

    def orthogonal_one(stack):
        iterate = stack[None]
        iterate = iterate * lax.rsqrt(lax.optimization_barrier(jnp.sum(iterate * iterate, axis=(1, 2), keepdims=True)) + 1e-06)
        for step in range(ITERS):
            gram = jnp.einsum('mik,mjk->mij', iterate, iterate, precision=lax.Precision.HIGHEST)
            mixed = -4.775 * gram + 2.0315 * jnp.einsum('mij,mjk->mik', gram, gram, precision=lax.Precision.HIGHEST)
            iterate = 3.4445 * iterate + jnp.einsum('mij,mjk->mik', mixed, iterate, precision=lax.Precision.HIGHEST)
        return iterate[0]
    iterate = lax.map(orthogonal_one, new_momentum)
    new_weights = weight_stack - learn_rate * iterate
    return (new_weights, new_momentum)
```

```python
import functools

import jax
import jax.numpy as jnp
from jax import lax
from jax.experimental import pallas as pl
from jax.experimental.pallas import tpu as pltpu
from jax.sharding import PartitionSpec as P

ITERS = 5
CHUNKS = 4

hold_rate = 0.95
learn_rate = 1.0

MESH = pl.DeviceIdType.MESH


def mul(a, b):
    return lax.dot_general(
        a, b, (((1,), (0,)), ((), ())),
        precision=lax.Precision.HIGHEST, preferred_element_type=jnp.float32,
    )


def mul_t(a, b):
    return lax.dot_general(
        a, b, (((1,), (1,)), ((), ())),
        precision=lax.Precision.HIGHEST, preferred_element_type=jnp.float32,
    )


def transform(packed, side):
    wide = 2 * side
    row = lax.broadcasted_iota(jnp.int32, (side, wide), 0)
    lane = lax.broadcasted_iota(jnp.int32, (side, wide), 1)
    first = lane < side
    scales = [
        lax.rsqrt(
            jnp.sum(
                jnp.sum(jnp.where(lane == row + at, packed, 0.0), axis=1, keepdims=True),
                axis=0, keepdims=True,
            ) + 1e-06
        )
        for at in (0, side)
    ]
    scale = jnp.where(first, scales[0], scales[1])
    scaled = packed * scale * scale
    gram = jnp.concatenate(
        [jnp.where(first, scaled, 0.0), jnp.where(first, 0.0, scaled)], axis=0
    )
    eye = lax.broadcasted_iota(jnp.int32, (wide, wide), 0) == lax.broadcasted_iota(
        jnp.int32, (wide, wide), 1
    )
    total = None
    for step in range(ITERS):
        factor = jnp.where(eye, 3.4445, 0.0) + (-4.775 * gram + 2.0315 * mul(gram, gram))
        total = factor if total is None else mul(factor, total)
        if step < ITERS - 1:
            gram = mul(factor, mul(factor, gram))
    return total * jnp.concatenate([scale, scale], axis=0)


def kernel(
    rows, cols, chunks, mom, back, held, made, mine, theirs, total, pair_buf,
    out_send, out_recv, gram_send, gram_recv, ret_send, ret_recv, own_sem,
):
    me, col = lax.axis_index("rows"), lax.axis_index("cols")
    _, mats, share, width = held.shape
    side = rows * share
    count = mats // chunks
    pairs = count // 2

    def row_peer(k):
        return lax.rem(me + k, rows)

    def col_peer(k):
        return lax.rem(col + k, cols)

    barrier = pltpu.get_barrier_semaphore()
    for k in range(1, rows):
        pl.semaphore_signal(barrier, inc=1, device_id=(row_peer(k), col), device_id_type=MESH)
    for k in range(1, cols):
        pl.semaphore_signal(barrier, inc=1, device_id=(me, col_peer(k)), device_id_type=MESH)
    pl.semaphore_wait(barrier, rows + cols - 2)

    def outgoing(c, k):
        to = row_peer(k)
        return pltpu.make_async_remote_copy(
            src_ref=mom.at[pl.ds(to * mats + c * count, count)],
            dst_ref=held.at[me, pl.ds(c * count, count)],
            send_sem=out_send.at[c, k - 1],
            recv_sem=out_recv.at[c, k - 1],
            device_id=(to, col),
            device_id_type=MESH,
        )

    def grams(c, k):
        return pltpu.make_async_remote_copy(
            src_ref=mine.at[pl.ds(c * pairs, pairs)],
            dst_ref=theirs.at[k - 1, pl.ds(c * pairs, pairs)],
            send_sem=gram_send.at[c, k - 1],
            recv_sem=gram_recv.at[c, k - 1],
            device_id=(me, col_peer(k)),
            device_id_type=MESH,
        )

    def returning(c, k):
        to = row_peer(k)
        return pltpu.make_async_remote_copy(
            src_ref=made.at[to, pl.ds(c * count, count)],
            dst_ref=back.at[pl.ds(me * mats + c * count, count)],
            send_sem=ret_send.at[c, k - 1],
            recv_sem=ret_recv.at[c, k - 1],
            device_id=(to, col),
            device_id_type=MESH,
        )

    def own_back(c):
        return pltpu.make_async_copy(
            made.at[me, pl.ds(c * count, count)],
            back.at[pl.ds(me * mats + c * count, count)],
            own_sem.at[c + 1],
        )

    own_in = pltpu.make_async_copy(mom.at[pl.ds(me * mats, mats)], held.at[me], own_sem.at[0])

    @pl.loop(0, chunks)
    def _(c):
        for k in range(1, rows):
            outgoing(c, k).start()

    own_in.start()
    own_in.wait()

    def load_pair(m):
        if share % 8 == 0:
            return jnp.concatenate(
                [held[:, m + at].reshape(side, width) for at in (0, 1)], axis=0
            )
        for at in (0, 1):
            for s in range(rows):
                pair_buf[pl.ds(at * side + s * share, share), :] = held[s, m + at]
        return pair_buf[...]

    def store_pair(m, value):
        if share % 8 == 0:
            for at in (0, 1):
                made[:, m + at] = value[at * side:(at + 1) * side].reshape(rows, share, width)
            return
        pair_buf[...] = value
        for at in (0, 1):
            for s in range(rows):
                made[s, m + at] = pair_buf[pl.ds(at * side + s * share, share), :]

    @pl.loop(0, chunks)
    def _(c):
        for k in range(1, rows):
            outgoing(c, k).wait_recv()

        @pl.loop(0, pairs)
        def _(p):
            x = load_pair(c * count + 2 * p)
            both = mul_t(x, x)
            lane = lax.broadcasted_iota(jnp.int32, (side, 2 * side), 1)
            mine[c * pairs + p] = jnp.where(lane < side, both[:side], both[side:])

        for k in range(1, cols):
            grams(c, k).start()
        for k in range(1, cols):
            grams(c, k).wait_recv()

        packed = []
        for p in range(pairs):
            at = c * pairs + p
            one = mine[at]
            for k in range(1, cols):
                one = one + theirs[k - 1, at]
            packed.append(one)
        for p, one in enumerate(packed):
            total[p] = transform(one, side)

        @pl.loop(0, pairs)
        def _(p):
            m = c * count + 2 * p
            store_pair(m, mul(total[p], load_pair(m)))

        for k in range(1, rows):
            returning(c, k).start()
        own_back(c).start()

    @pl.loop(0, chunks)
    def _(c):
        for k in range(1, rows):
            returning(c, k).wait_recv()
            returning(c, k).wait_send()
            outgoing(c, k).wait_send()
        for k in range(1, cols):
            grams(c, k).wait_send()
        own_back(c).wait()


def exchange_and_iterate(new_momentum, rows, cols):
    every, share, width = new_momentum.shape
    mats = every // rows
    side = rows * share
    chunks = CHUNKS
    pairs = mats // chunks // 2
    f32, dma = jnp.float32, pltpu.SemaphoreType.DMA
    return pl.pallas_call(
        functools.partial(kernel, rows, cols, chunks),
        out_shape=jax.ShapeDtypeStruct((every, share, width), f32),
        in_specs=[pl.BlockSpec(memory_space=pl.ANY)],
        out_specs=pl.BlockSpec(memory_space=pl.ANY),
        scratch_shapes=[
            pltpu.VMEM((rows, mats, share, width), f32),
            pltpu.VMEM((rows, mats, share, width), f32),
            pltpu.VMEM((mats // 2, side, 2 * side), f32),
            pltpu.VMEM((cols - 1, mats // 2, side, 2 * side), f32),
            pltpu.VMEM((pairs, 2 * side, 2 * side), f32),
            pltpu.VMEM((2 * side, width), f32),
            dma((chunks, rows - 1)),
            dma((chunks, rows - 1)),
            dma((chunks, cols - 1)),
            dma((chunks, cols - 1)),
            dma((chunks, rows - 1)),
            dma((chunks, rows - 1)),
            dma((chunks + 1,)),
        ],
        compiler_params=pltpu.CompilerParams(
            collective_id=0, has_side_effects=True, vmem_limit_bytes=48 * 2**20
        ),
        name="exchange_and_iterate",
    )(new_momentum)


def solution(mesh):
    rows, cols = mesh.shape["rows"], mesh.shape["cols"]

    def on_device(grad_stack, moment_stack, weight_stack):
        new_momentum = hold_rate * moment_stack + grad_stack
        back = exchange_and_iterate(new_momentum, rows, cols)
        new_weights = weight_stack - learn_rate * back
        return (new_weights, new_momentum)

    placed = P(None, "rows", "cols")
    return jax.shard_map(
        on_device,
        mesh=mesh,
        in_specs=(placed, placed, placed),
        out_specs=(placed, placed),
        check_vma=False,
    )
```
